256 devices in a mesh: gx: 8 (over x, core), gy: 4 (over y), gz: 8 (over z).
Axes of the slice: x: 4, y: 4, z: 8, core: 2. Of those that a mesh axis runs over, the one named last changes fastest.
Arguments:
- dual_rhs: float32 [8, 4, 8, 3, 300, 128], P('gx', 'gy', 'gz'), may hold values from -6 to 6
- local_flex: bfloat16 [8, 4, 8, 1800, 1800], P('gx', 'gy', 'gz'), as said below
- corner_coupling: bfloat16 [8, 4, 8, 24, 1800], P('gx', 'gy', 'gz'), may hold values from -0.375 to 0.375
- face_stiffness: bfloat16 [8, 4, 8, 6, 300, 300], P('gx', 'gy', 'gz'), as said below
- coarse_inverse: bfloat16 [441, 441], replicated, as said below
- corner_ids: int32 [8, 4, 8, 8], P('gx', 'gy', 'gz'), may hold values from -1 to 146, as said below
Outputs:
- multipliers: float32 [8, 4, 8, 3, 300, 128], P('gx', 'gy', 'gz')
- residual: float32 [8, 4, 8, 3, 300, 128], P('gx', 'gy', 'gz')
The draws below stay inside these ranges and needn't reach their ends.
Inputs may be any that keep to these rules, and one draw needn't show every extreme that they name: `local_flex`: each subdomain's matrix is symmetric positive definite. `face_stiffness`: each face block is symmetric positive definite. `coarse_inverse`: symmetric positive definite. `corner_ids`: entry k = 4 kx + 2 ky + kz of subdomain (i, j, l) is the number of the corner at lattice point (i + kx, j + ky, l + kz) when that point has all coordinates strictly between 0 and the subdomain counts, else -1; the 147 interior corners are numbered by a permutation, so subdomains sharing a corner name the same node.
All inputs are finite; a program needn't handle non-finite values.
Results may differ from the reference program's by a relative error of at most 0.04.
Values may be sent and summed in bfloat16 or wider, within the bound.
No kernel may reach another device: no remote copies, remote signals or barrier semaphores. Data moves between devices by JAX's collectives and lax.ppermute only.
A program may use at most 64 MiB of HBM per device.

```python
import math
import jax
import jax.numpy as jnp
from jax import lax

P_SIZE = 300
R = 128
ITERS = 3
SX = 8
SY = 4
SZ = 8
Q = 1800
NNODE = 147
NC = 441


def spd_block(block_key, order, lowest, highest, spread):
    first, second = jax.random.split(block_key, 2)
    diagonal = jax.random.uniform(first, (order,), jnp.float32, lowest, highest)
    gaussian = jax.random.normal(second, (order, order), jnp.float32)
    matrix = (gaussian + gaussian.T) * (spread / math.sqrt(2.0 * order)) + jnp.diag(diagonal)
    return matrix


def draw_local_flex(key, part):
    base_key = jax.random.fold_in(key, 11)

    def one_block(block_index):
        return spd_block(jax.random.fold_in(base_key, block_index), Q, 0.7, 1.8, 0.28).astype(jnp.bfloat16)
    matrices = lax.map(one_block, jnp.arange(SX * SY * SZ))
    return matrices.reshape(SX, SY, SZ, Q, Q)


def draw_face_stiffness(key, part):
    base_key = jax.random.fold_in(key, 23)

    def one_block(block_index):
        return spd_block(jax.random.fold_in(base_key, block_index), P_SIZE, 1.0, 2.5, 0.4).astype(jnp.bfloat16)
    matrices = lax.map(one_block, jnp.arange(SX * SY * SZ * 6))
    return matrices.reshape(SX, SY, SZ, 6, P_SIZE, P_SIZE)


def draw_coarse_inverse(key, part):
    return spd_block(jax.random.fold_in(key, 37), NC, 0.6, 1.4, 0.24).astype(jnp.bfloat16)


def draw_corner_ids(key, part):
    numbering = jax.random.permutation(jax.random.fold_in(key, 53), NNODE).astype(jnp.int32)
    corner = jnp.arange(8, dtype=jnp.int32)
    point_x = jnp.arange(SX, dtype=jnp.int32)[:, None, None, None] + corner // 4
    point_y = jnp.arange(SY, dtype=jnp.int32)[None, :, None, None] + corner // 2 % 2
    point_z = jnp.arange(SZ, dtype=jnp.int32)[None, None, :, None] + corner % 2
    inside = (point_x >= 1) & (point_x <= SX - 1) & (point_y >= 1) & (point_y <= SY - 1) & (point_z >= 1) & (point_z <= SZ - 1)
    lattice_index = ((point_x - 1) * (SY - 1) + (point_y - 1)) * (SZ - 1) + (point_z - 1)
    lattice_index = jnp.where(inside, lattice_index, 0)
    return jnp.where(inside, numbering[lattice_index], -1).astype(jnp.int32)


def level_of(rng, shape, cuts, low, top_value):
    factor_of, own = 1.0, jax.random.fold_in(rng, 6)
    for dim, parts in cuts:
        steps = jnp.exp(jax.random.uniform(jax.random.fold_in(own, dim), (parts,), jnp.float32, low / len(cuts), top_value / len(cuts)))
        factor_of = factor_of * jnp.repeat(steps, shape[dim] // parts).reshape([-1 if axis == dim else 1 for axis in range(len(shape))])
    return factor_of


def normal_values(stream_key, shape, deviation, bound, shards=(), held_as=jnp.bfloat16):
    level = level_of(stream_key, shape, shards, -0.22, 0.18) if shards else 1.0
    entries = jax.random.normal(stream_key, shape, jnp.float32) * deviation * level
    return jnp.minimum(jnp.maximum(entries, -bound), bound).astype(held_as)


def setup_inputs(seed: int = 0) -> dict:
    streams_of = jax.random.split(jax.random.key(seed), 7)
    dual_rhs = normal_values(streams_of[0], (SX, SY, SZ, 3, P_SIZE, R), 1.0, 6.0, ((0, 8), (1, 4), (2, 8)), jnp.float32)
    local_flex = draw_local_flex(jax.random.fold_in(streams_of[6], 71), 0)
    corner_coupling = normal_values(streams_of[2], (SX, SY, SZ, 24, Q), (Q // 8) ** -0.5, 0.375, ((0, 8), (1, 4), (2, 8)))
    face_stiffness = draw_face_stiffness(jax.random.fold_in(streams_of[6], 71), 0)
    coarse_inverse = draw_coarse_inverse(jax.random.fold_in(streams_of[6], 71), 0)
    corner_ids = draw_corner_ids(jax.random.fold_in(streams_of[6], 71), 0)
    return {"dual_rhs": dual_rhs, "local_flex": local_flex, "corner_coupling": corner_coupling, "face_stiffness": face_stiffness, "coarse_inverse": coarse_inverse, "corner_ids": corner_ids}


def reference(dual_rhs, local_flex, corner_coupling, face_stiffness, coarse_inverse, corner_ids):
    block_count = SX * SY * SZ
    grid_x = jnp.broadcast_to(jnp.arange(SX)[:, None, None], (SX, SY, SZ))
    grid_y = jnp.broadcast_to(jnp.arange(SY)[None, :, None], (SX, SY, SZ))
    grid_z = jnp.broadcast_to(jnp.arange(SZ)[None, None, :], (SX, SY, SZ))
    face_mask = jnp.stack([grid_x > 0, grid_x < SX - 1, grid_y > 0, grid_y < SY - 1, grid_z > 0, grid_z < SZ - 1], axis=-1).astype(jnp.float32)
    expanded = face_mask[..., None, None]
    face_sign = jnp.array([-1.0, 1.0, -1.0, 1.0, -1.0, 1.0], jnp.float32)[:, None, None]

    def duplicate(owned):
        face_list = []
        for axis_pos in range(3):
            plus_face = owned[:, :, :, axis_pos]
            face_list.append(jnp.roll(plus_face, 1, axis=axis_pos))
            face_list.append(plus_face)
        return jnp.stack(face_list, axis=3) * expanded

    def face_jump(values):
        face_list = []
        for axis_pos in range(3):
            minus_face = values[:, :, :, 2 * axis_pos]
            plus_face = values[:, :, :, 2 * axis_pos + 1]
            face_list.append(jnp.roll(plus_face, 1, axis=axis_pos) - minus_face)
            face_list.append(plus_face - jnp.roll(minus_face, -1, axis=axis_pos))
        return jnp.stack(face_list, axis=3) * expanded

    def face_product(operands):
        return jnp.dot(operands[0], operands[1], preferred_element_type=jnp.float32)

    stiff_flat = face_stiffness.reshape(block_count * 6, P_SIZE, P_SIZE)

    def precondition(dual):
        halved = (0.5 * face_sign * dual).astype(jnp.bfloat16)
        products = lax.map(face_product, (stiff_flat, halved.reshape(block_count * 6, P_SIZE, R)))
        return 0.5 * face_jump(products.reshape(SX, SY, SZ, 6, P_SIZE, R))

    flex_flat = local_flex.reshape(block_count, Q, Q)
    coupling_flat = corner_coupling.reshape(block_count, 24, Q)
    coupling_wide = coupling_flat.astype(jnp.float32)
    id_rows = corner_ids.reshape(block_count, 8)
    dof_ids = jnp.where(id_rows[:, :, None] >= 0, 3 * id_rows[:, :, None] + jnp.arange(3, dtype=jnp.int32)[None, None, :], NC).astype(jnp.int32).reshape(block_count, 24)

    def local_solve(operands):
        flex_block, coupling_block, signed_block = operands
        return (jnp.dot(flex_block, signed_block, preferred_element_type=jnp.float32),
                jnp.dot(coupling_block, signed_block, preferred_element_type=jnp.float32))

    def dual_operator(direction):
        signed = (face_sign * direction).astype(jnp.bfloat16).reshape(block_count, Q, R)
        local_image, corner_part = lax.map(local_solve, (flex_flat, coupling_flat, signed))
        coarse_rhs = jax.ops.segment_sum(corner_part.reshape(block_count * 24, R), dof_ids.reshape(-1), num_segments=NC + 1)[:NC]
        coarse_sol = jnp.dot(coarse_inverse, coarse_rhs.astype(jnp.bfloat16), preferred_element_type=jnp.float32)
        padded = jnp.concatenate([coarse_sol, jnp.zeros((1, R), jnp.float32)], axis=0)
        corner_sol = padded[dof_ids]
        displaced = local_image + jnp.einsum("nkq,nkr->nqr", coupling_wide, corner_sol, precision=lax.Precision.HIGHEST)
        curvature = jnp.sum(signed.astype(jnp.float32) * displaced, axis=(0, 1))
        return face_jump(displaced.reshape(SX, SY, SZ, 6, P_SIZE, R)), curvature

    def inner(left, right):
        return jnp.sum(left[:, :, :, 1::2] * right[:, :, :, 1::2], axis=(0, 1, 2, 3, 4))

    residual = duplicate(dual_rhs)
    multiplier = jnp.zeros_like(residual)
    precond_res = precondition(residual)
    rho_now = inner(residual, precond_res)
    direction = precond_res
    for iteration in range(ITERS):
        image, curvature = dual_operator(direction)
        step_size = rho_now / curvature
        multiplier = multiplier + step_size * direction
        residual = residual - step_size * image
        if iteration + 1 < ITERS:
            precond_res = precondition(residual)
            rho_next = inner(residual, precond_res)
            direction = precond_res + (rho_next / rho_now) * direction
            rho_now = rho_next
    return multiplier[:, :, :, 1::2], residual[:, :, :, 1::2]
```

```python
import jax
import jax.numpy as jnp
import numpy as np
from jax import lax
from jax.sharding import Mesh
from jax.sharding import PartitionSpec as P

ITERS = 3
GX = ("gx_0", "gx_1")
PLANE = ("gx_0", "gx_1", "gy")
BF16 = jnp.bfloat16
F32 = jnp.float32
MSG_ROWS = 32


def shifted(value, axis, up):
    size = lax.axis_size(axis)
    pairs = [(i, i + 1) for i in range(size - 1)]
    return lax.ppermute(value, axis, pairs if up else [(j, i) for i, j in pairs])


def from_everyone(value, axes):
    copies = jnp.broadcast_to(value, (lax.axis_size(axes), *value.shape))
    return lax.all_to_all(copies, axes, split_axis=0, concat_axis=0, tiled=True)


def split_pair(value):
    high = value.astype(BF16)
    low = (value - high.astype(F32)).astype(BF16)
    return high, low


def plane_sum_matrix(sx, sy, plane_rows):
    matrix = np.zeros((plane_rows, sx * sy * MSG_ROWS), np.float32)
    inner = (sx - 1) * (sy - 1) * 6
    for i in range(sx):
        for j in range(sy):
            base = (i * sy + j) * MSG_ROWS
            for kx in range(2):
                for ky in range(2):
                    a, b = i + kx, j + ky
                    if 1 <= a <= sx - 1 and 1 <= b <= sy - 1:
                        for kz in range(2):
                            for d in range(3):
                                row = (((a - 1) * (sy - 1) + b - 1) * 2 + kz) * 3 + d
                                matrix[row, base + 3 * (4 * kx + 2 * ky + kz) + d] = 1
            for n in range(3):
                matrix[inner + n, base + 24 + n] = 1
                matrix[inner + n, base + 27 + n] = 1
            matrix[inner + 3, base + 30] = 1
    return matrix


def line_sum_matrix(sx, sy, sz, plane_rows, coarse_rows, total_rows):
    matrix = np.zeros((total_rows, sz * plane_rows), np.float32)
    inner = (sx - 1) * (sy - 1) * 6
    for layer in range(sz):
        base = layer * plane_rows
        for point in range((sx - 1) * (sy - 1)):
            for kz in range(2):
                c = layer + kz
                if 1 <= c <= sz - 1:
                    for d in range(3):
                        row = 3 * (point * (sz - 1) + c - 1) + d
                        matrix[row, base + (point * 2 + kz) * 3 + d] = 1
        for n in range(3):
            matrix[coarse_rows + n, base + inner + n] = 1
            matrix[coarse_rows + n, base + inner + 3 + n] = 1
    return matrix


def body(dual_rhs, local_flex, corner_coupling, face_stiffness, coarse_inverse, corner_ids):
    owned_rhs = dual_rhs[0, 0, 0]
    flex = local_flex[0, 0, 0]
    coupling = corner_coupling[0, 0, 0]
    stiffness = face_stiffness[0, 0, 0]
    corner_list = corner_ids[0, 0, 0]
    faces, width, columns = (stiffness.shape[0], stiffness.shape[1], owned_rhs.shape[2])
    coarse_rows = coarse_inverse.shape[0]
    sx, sy, sz = (lax.axis_size(GX), lax.axis_size("gy"), lax.axis_size("gz"))
    axes = (GX, "gy", "gz")
    px, py, pz = (lax.axis_index(GX), lax.axis_index("gy"), lax.axis_index("gz"))
    sign = jnp.array([-1.0, 1.0, -1.0, 1.0, -1.0, 1.0], F32)[:, None, None]
    mask = jnp.stack(
        [px > 0, px < sx - 1, py > 0, py < sy - 1, pz > 0, pz < sz - 1]
    ).astype(F32)[:, None, None]

    inner_rows = (sx - 1) * (sy - 1) * 6
    plane_rows = -(-(inner_rows + 7) // 8) * 8
    total_rows = -(-(coarse_rows + 3) // 8) * 8
    plane_sum = jnp.asarray(plane_sum_matrix(sx, sy, plane_rows), BF16)
    line_sum = jnp.asarray(
        line_sum_matrix(sx, sy, sz, plane_rows, coarse_rows, total_rows), BF16
    )

    coupling_faces = coupling.reshape(24, faces, width)
    beyond, far_coupling, far_rhs = [None] * 6, [None] * 6, [None] * 3
    rhs_low = owned_rhs.astype(BF16)
    for a, axis in enumerate(axes):
        up = jnp.concatenate(
            [stiffness[2 * a + 1], coupling_faces[:, 2 * a + 1].T, rhs_low[a]], axis=1
        )
        down = jnp.concatenate([stiffness[2 * a], coupling_faces[:, 2 * a].T], axis=1)
        before = shifted(up, axis, True)
        after = shifted(down, axis, False)
        beyond[2 * a], beyond[2 * a + 1] = before[:, :width], after[:, :width]
        far_coupling[2 * a] = before[:, width : width + 24]
        far_coupling[2 * a + 1] = after[:, width:]
        far_rhs[a] = before[:, width + 24 :].astype(F32)
    beyond = jnp.stack(beyond)
    signed_own = jnp.stack([coupling_faces[:, f].T for f in range(6)])
    spread = jnp.concatenate([signed_own, -jnp.stack(far_coupling)], axis=2)
    spread = (spread * (sign * mask).astype(BF16)).astype(BF16)
    spread = jnp.concatenate([spread, spread], axis=2)

    moves = np.array(
        [[0, 0, 0], [-1, 0, 0], [1, 0, 0], [0, -1, 0], [0, 1, 0], [0, 0, -1], [0, 0, 1]]
    )
    corner = np.arange(8)
    offsets = np.stack([corner // 4, corner // 2 % 2, corner % 2], axis=1)
    points = np.repeat((moves[:, None, :] + offsets[None, :, :]).reshape(-1, 3), 3, axis=0)
    qx, qy, qz = (px + points[:, 0], py + points[:, 1], pz + points[:, 2])
    inside = (qx > 0) & (qx < sx) & (qy > 0) & (qy < sy) & (qz > 0) & (qz < sz)
    lattice = ((qx - 1) * (sy - 1) + (qy - 1)) * (sz - 1) + (qz - 1)
    used = jnp.where(inside, 3 * lattice + np.tile(np.arange(3), 56), -1)
    select = (used[:, None] == jnp.arange(coarse_rows)[None, :]).astype(BF16)

    def precondition(dual):
        low = dual.astype(BF16)
        own = jnp.einsum("fij,fjr->fir", stiffness, low, preferred_element_type=F32)
        far = jnp.einsum("fij,fjr->fir", beyond, low, preferred_element_type=F32)
        return 0.25 * mask * (own + far)

    def exchange(corner_part, inner, number_row):
        highs, lows = zip(*[split_pair(v) for v in inner])
        message = jnp.concatenate(
            [corner_part.astype(BF16), jnp.stack(highs), jnp.stack(lows), number_row]
        )
        plane = from_everyone(message, PLANE).reshape(-1, columns)
        plane = jnp.dot(plane_sum, plane, preferred_element_type=F32)
        highs, lows = split_pair(plane[inner_rows : inner_rows + 3])
        numbers = plane[inner_rows + 3 : inner_rows + 4].astype(BF16)
        spare = jnp.zeros((plane_rows - inner_rows - 7, columns), BF16)
        message = jnp.concatenate([plane[:inner_rows].astype(BF16), highs, lows, numbers, spare])
        line = from_everyone(message, "gz")
        total = jnp.dot(line_sum, line.reshape(-1, columns), preferred_element_type=F32)
        return total[:coarse_rows], total[coarse_rows : coarse_rows + 3], line[:, inner_rows + 6]

    residual = jnp.stack(
        [far_rhs[0], owned_rhs[0], far_rhs[1], owned_rhs[1], far_rhs[2], owned_rhs[2]]
    ) * mask
    place = px * sy + py
    number_row = jnp.where(jnp.arange(columns) == place, corner_list[0], 0).astype(BF16)
    number_row = jnp.stack([number_row, jnp.zeros_like(number_row)])
    blank_row = jnp.zeros_like(number_row)
    zero = jnp.zeros((columns,), F32)

    for iteration in range(ITERS):
        last = iteration + 1 == ITERS
        precond = precondition(residual)
        signed = (sign * precond).astype(BF16).reshape(faces * width, columns)
        image = jnp.dot(flex, signed, preferred_element_type=F32)
        corner_part = jnp.dot(coupling, signed, preferred_element_type=F32)
        image_low = image.astype(BF16).reshape(faces, width, columns)
        far_image = [None] * 6
        for a, axis in enumerate(axes):
            far_image[2 * a + 1] = shifted(image_low[2 * a], axis, False)
            if not last:
                far_image[2 * a] = shifted(image_low[2 * a + 1], axis, True)
        rho = jnp.sum(residual[1::2] * precond[1::2], axis=(0, 1))
        wide = signed.astype(F32)
        own_energy = jnp.sum(wide * image, axis=0)
        cross_energy = jnp.sum(wide * image_old, axis=0) if iteration else zero
        coarse_rhs, inner, numbers = exchange(
            corner_part, (rho, own_energy, cross_energy), blank_row if iteration else number_row
        )
        rho, own_energy, cross_energy = inner[0], inner[1], inner[2]
        if iteration == 0:
            order = numbers[:, : sx * sy].astype(F32).reshape(sz, sx, sy)[1:, 1:, 1:]
            order = jnp.transpose(order, (1, 2, 0)).reshape(-1).astype(jnp.int32)
            dofs = (3 * order[:, None] + jnp.arange(3)[None, :]).reshape(-1)
            pick = (dofs[:, None] == jnp.arange(coarse_rows)[None, :]).astype(BF16)
            inverse = jnp.dot(pick, coarse_inverse, preferred_element_type=F32).astype(BF16)
            inverse = lax.dot_general(
                inverse, pick, (((1,), (1,)), ((), ())), preferred_element_type=F32
            ).astype(BF16)
            chosen = jnp.dot(select, inverse, preferred_element_type=F32).astype(BF16)
        coarse_low = coarse_rhs.astype(BF16)
        coarse_sol = jnp.dot(inverse, coarse_low, preferred_element_type=F32)
        corner_sol = jnp.dot(chosen, coarse_low, preferred_element_type=F32)
        high, low = split_pair(corner_sol)
        high, low = high.reshape(7, 24, columns), low.reshape(7, 24, columns)

        def moved_face(f):
            corners = jnp.concatenate([high[0], high[1 + f], low[0], low[1 + f]])
            return jnp.dot(spread[f], corners, preferred_element_type=F32)

        def jump(f):
            near, far = image_low[f].astype(F32), far_image[f].astype(F32)
            return sign[f] * mask[f] * (near - far) + moved_face(f)

        chosen_faces = range(1, 6, 2) if last else range(6)
        operated = jnp.stack([jump(f) for f in chosen_faces])
        plus = precond[1::2]
        if iteration == 0:
            direction, image_old, operated_old = plus, image, operated
            coarse_rhs_old, coarse_sol_old, energy = coarse_rhs, coarse_sol, own_energy
        else:
            ratio = rho / rho_old
            direction = plus + ratio * direction
            operated_old = operated + ratio * (operated_old[1::2] if last else operated_old)
            image_old = image + ratio * image_old
            coarse_rhs_old = coarse_rhs + ratio * coarse_rhs_old
            coarse_sol_old = coarse_sol + ratio * coarse_sol_old
            energy = own_energy + 2.0 * ratio * cross_energy + ratio * ratio * energy
        rho_old = rho
        curvature = energy + jnp.sum(coarse_rhs_old * coarse_sol_old, axis=0)
        step = rho / curvature
        multiplier = step * direction + (multiplier if iteration else 0.0)
        residual = (residual[1::2] if last else residual) - step * operated_old
    return (multiplier[None, None, None], residual[None, None, None])


def solution(mesh):
    torus = Mesh(
        mesh.devices.reshape(4, 2, mesh.shape["gy"], mesh.shape["gz"]), ("gx_0", "gx_1", "gy", "gz")
    )
    in_specs = (
        P(GX, "gy", "gz", None, None, None),
        P(GX, "gy", "gz", None, None),
        P(GX, "gy", "gz", None, None),
        P(GX, "gy", "gz", None, None, None),
        P(),
        P(GX, "gy", "gz", None),
    )
    out_specs = (P(GX, "gy", "gz", None, None, None), P(GX, "gy", "gz", None, None, None))
    return jax.shard_map(body, mesh=torus, in_specs=in_specs, out_specs=out_specs, check_vma=False)
```
